32 devices in a mesh: inp: 8 (over z, y), tm: 4 (over x, core).
Axes of the slice: x: 2, y: 2, z: 4, core: 2. Of those that a mesh axis runs over, the one named last changes fastest.
Arguments:
- voltages: bfloat16 [1024, 262144], P('inp', 'tm'), may hold values from -6 to 6
- pfb_coeff: float32 [16, 512], replicated, may hold values from -1.5 to 1.5
Outputs:
- visibilities: float32 [32, 2, 1024, 1024], P(('inp', 'tm'))
The draws below stay inside these ranges and needn't reach their ends.
All inputs are finite; a program needn't handle non-finite values.
Results may differ from the reference program's by a relative error of at most 0.0029.
Values may be sent and summed in bfloat16 or wider, within the bound.
No kernel may reach another device: no remote copies, remote signals or barrier semaphores. Data moves between devices by JAX's collectives and lax.ppermute only.
A program may use at most 128 MiB of HBM per device.

```python
import math
import jax
import jax.numpy as jnp
from jax import lax

INPUTS = 1024
FFT_LEN = 512
TAPS = 16
CHAN = 32
SPECTRA = 512


def shard_levels(stream_key, extent, shards, low, high):
    def one(position, blocks):
        heights = jax.random.uniform(jax.random.fold_in(jax.random.fold_in(stream_key, 6), position), (blocks,), jnp.float32, low / len(shards), high / len(shards))
        return jnp.repeat(jnp.exp(heights), extent[position] // blocks).reshape((-1,) + (1,) * (len(extent) - position - 1))

    level = one(*shards[0])
    for cut in shards[1:]:
        level = level * one(*cut)
    return level


def bell_draw(key, dims, deviation, limit, shards=(), kind=jnp.bfloat16):
    result = jax.random.normal(key, dims, jnp.float32) * deviation
    if len(shards) > 0:
        result = shard_levels(key, dims, shards, -0.22, 0.18) * result
    return jnp.clip(result, min=-limit, max=limit).astype(kind)


def setup_inputs(seed: int = 0) -> dict:
    keys = jax.random.split(jax.random.key(seed), 3)
    voltages = bell_draw(keys[0], (INPUTS, SPECTRA * FFT_LEN), 1.0, 6.0, ((0, 8), (1, 4)))
    pfb_coeff = bell_draw(keys[1], (TAPS, FFT_LEN), TAPS ** -0.5, 1.5, (), jnp.float32)
    return dict(voltages=voltages, pfb_coeff=pfb_coeff)


def reference(voltages, pfb_coeff):
    input_block = math.gcd(INPUTS, 32)
    blocks = voltages.reshape(INPUTS // input_block, input_block, SPECTRA, FFT_LEN)

    def channelize(input_group):
        padded = jnp.concatenate([jnp.zeros((input_block, TAPS - 1, FFT_LEN), input_group.dtype), input_group], axis=1)
        filtered = jnp.zeros((input_block, SPECTRA, FFT_LEN), jnp.float32)
        for tap_index in range(TAPS):
            filtered = filtered + pfb_coeff[tap_index][None, None, :] * padded[:, tap_index:tap_index + SPECTRA, :].astype(jnp.float32)
        spectrum = jnp.fft.rfft(filtered, axis=-1)[:, :, :CHAN]
        norm_scale = 1.0 / math.sqrt(FFT_LEN)
        real_part = (jnp.real(spectrum) * norm_scale).astype(jnp.bfloat16)
        imag_part = (jnp.imag(spectrum) * norm_scale).astype(jnp.bfloat16)
        return jnp.stack([real_part, imag_part], axis=0)
    channelized = lax.map(channelize, blocks)
    channelized = jnp.transpose(channelized, (4, 1, 0, 2, 3)).reshape(CHAN, 2, INPUTS, SPECTRA)

    def gram_matrix(chan_data):
        real_part = chan_data[0].astype(jnp.float32)
        imag_part = chan_data[1].astype(jnp.float32)
        same_pol = jnp.dot(real_part, real_part.T, precision=lax.Precision.HIGHEST, preferred_element_type=jnp.float32)
        same_pol = same_pol + jnp.dot(imag_part, imag_part.T, precision=lax.Precision.HIGHEST, preferred_element_type=jnp.float32)
        cross_term = jnp.dot(imag_part, real_part.T, precision=lax.Precision.HIGHEST, preferred_element_type=jnp.float32)
        return jnp.stack([same_pol, cross_term - cross_term.T], axis=0) * (1.0 / SPECTRA)
    return lax.map(gram_matrix, channelized)
```

```python
import functools
import math

import jax
import jax.numpy as jnp
import numpy as np
from jax import lax
from jax.experimental import pallas as pl
from jax.experimental.pallas import tpu as pltpu
from jax.sharding import PartitionSpec as P

CH_DEV = 1
STEP = 16
ROWS = 16
LANES = 128
VMEM_LIMIT = 60 * 1024 * 1024


def shifted(block, axis, distance):
    devices = range(lax.axis_size(axis))
    route = [(i - distance, i) for i in devices if i - distance in devices]
    return lax.ppermute(block, axis, route)


def dft_table(channels, length):
    samples = np.arange(length)
    angle = (np.arange(channels)[:, None] * samples[None, :] % length) * (2.0 * math.pi / length)
    table = np.stack([np.cos(angle), -np.sin(angle)], axis=1).reshape(2 * channels, length)
    table = (table / math.sqrt(length)).T
    high = table.astype(jnp.bfloat16)
    low = (table - high.astype(np.float64)).astype(jnp.bfloat16)
    both = np.concatenate([high, low], axis=1)
    return jnp.asarray(np.concatenate([both, both], axis=0))


def spectra_kernel(prev_ref, main_ref, coeff_ref, table_ref, out_ref, parts_ref, turn_ref, *, taps, length, offset):
    in_rows = main_ref.shape[0]
    width = out_ref.shape[0]
    tiles = length // LANES

    def block_at(position, row, lane):
        ref, first = (main_ref, position) if position >= 0 else (prev_ref, position + offset)
        return ref[pl.ds(row, ROWS), pl.ds(first * length + lane, LANES)].astype(jnp.float32)

    def filter_tile(index, carry):
        row = pl.multiple_of(index // tiles * ROWS, ROWS)
        lane = pl.multiple_of(index % tiles * LANES, LANES)
        gains = [coeff_ref[pl.ds(8 * j, 8), pl.ds(lane, LANES)] for j in range(taps)]
        sums = {}
        for position in range(1 - taps, STEP):
            block = block_at(position, row, lane)
            halves = [block[8 * k : 8 * k + 8] for k in range(ROWS // 8)]
            for j in range(taps):
                spectrum = position + taps - 1 - j
                if 0 <= spectrum < STEP:
                    terms = [gains[j] * half for half in halves]
                    if spectrum in sums:
                        terms = [s + t for s, t in zip(sums[spectrum], terms)]
                    sums[spectrum] = terms
            if position >= 0:
                total = jnp.concatenate(sums.pop(position), axis=0)
                high = total.astype(jnp.bfloat16)
                low = (total - high.astype(jnp.float32)).astype(jnp.bfloat16)
                target = pl.ds(position * in_rows + row, ROWS)
                parts_ref[target, pl.ds(lane, LANES)] = high
                parts_ref[target, pl.ds(length + lane, LANES)] = low
        return carry

    lax.fori_loop(0, in_rows // ROWS * tiles, filter_tile, 0)

    for spectrum in range(STEP):
        part = parts_ref[pl.ds(spectrum * in_rows, in_rows), :]
        product = jnp.dot(part, table_ref[...], preferred_element_type=jnp.float32).T
        turn_ref[pl.ds(spectrum, width, stride=STEP), :] = product[:width] + product[width:]
    out_ref[...] = turn_ref[...].reshape(width, STEP, in_rows).astype(jnp.bfloat16)


def spectra(previous, prev_index, voltages, first, count, coeff, table, length):
    taps = coeff.shape[0] // 8
    in_rows = voltages.shape[0]
    width = table.shape[1] // 2
    prev_cols, prev_map = prev_index
    body = functools.partial(spectra_kernel, taps=taps, length=length, offset=prev_cols // length)
    return pl.pallas_call(
        body,
        grid=(count // STEP,),
        in_specs=[
            pl.BlockSpec((in_rows, prev_cols), prev_map),
            pl.BlockSpec((in_rows, STEP * length), lambda k: (0, k + first // STEP)),
            pl.BlockSpec(coeff.shape, lambda k: (0, 0)),
            pl.BlockSpec(table.shape, lambda k: (0, 0)),
        ],
        out_specs=pl.BlockSpec((width, STEP, in_rows), lambda k: (0, k, 0)),
        out_shape=jax.ShapeDtypeStruct((width, count, in_rows), jnp.bfloat16),
        scratch_shapes=[
            pltpu.VMEM((STEP * in_rows, 2 * length), jnp.bfloat16),
            pltpu.VMEM((width * STEP, in_rows), jnp.float32),
        ],
        compiler_params=pltpu.CompilerParams(vmem_limit_bytes=VMEM_LIMIT),
    )(previous, voltages, coeff, table)


def correlate_kernel(*refs, groups_tm):
    received, (out_ref, stack_ref) = refs[:-2], refs[-2:]
    block = out_ref.shape[2]
    depth = stack_ref.shape[0]
    half = depth // 2

    @pl.when(pl.program_id(0) == 0)
    def _():
        at = 0
        for part in range(2):
            for ref in received:
                sources, _, count, in_rows = ref.shape
                for source in range(sources):
                    group, slab = divmod(source, groups_tm)
                    start = at + slab * count
                    stack_ref[start : start + count, group * in_rows : (group + 1) * in_rows] = ref[source, part]
                at += groups_tm * count

    row = pl.multiple_of(pl.program_id(0) * block, block)
    turned = stack_ref[:, pl.ds(row, block)].T
    crossed = jnp.concatenate([turned[:, half:], -turned[:, :half]], axis=1)
    scale = 2.0 / depth
    everything = stack_ref[...]
    out_ref[0, 0] = jnp.dot(turned, everything, preferred_element_type=jnp.float32) * scale
    out_ref[0, 1] = jnp.dot(crossed, everything, preferred_element_type=jnp.float32) * scale


def correlate(received, groups_tm):
    sources, _, _, in_rows = received[0].shape
    inputs = sources // groups_tm * in_rows
    depth = 2 * groups_tm * sum(r.shape[2] for r in received)
    block = math.gcd(inputs, LANES)
    return pl.pallas_call(
        functools.partial(correlate_kernel, groups_tm=groups_tm),
        grid=(inputs // block,),
        in_specs=[pl.BlockSpec(r.shape, lambda k: (0, 0, 0, 0)) for r in received],
        out_specs=pl.BlockSpec((1, 2, block, inputs), lambda k: (0, 0, k, 0)),
        out_shape=jax.ShapeDtypeStruct((1, 2, inputs, inputs), jnp.float32),
        scratch_shapes=[pltpu.VMEM((depth, inputs), jnp.bfloat16)],
        compiler_params=pltpu.CompilerParams(vmem_limit_bytes=VMEM_LIMIT),
    )(*received)


def per_device(voltages, pfb_coeff):
    in_rows = voltages.shape[0]
    taps, length = pfb_coeff.shape
    spec_dev = voltages.shape[1] // length
    groups_tm = lax.axis_size("tm")
    devices = lax.axis_size("inp") * groups_tm
    channels = CH_DEV * devices
    tail = (taps - 1) * length
    history = shifted(voltages[:, voltages.shape[1] - tail :], "tm", 1)
    coeff = jnp.repeat(pfb_coeff, 8, axis=0)
    table = dft_table(channels, length)

    later = spectra(
        voltages, (STEP * length, lambda k: (0, k)), voltages, STEP, spec_dev - STEP, coeff, table, length
    )
    early = spectra(history, (tail, lambda k: (0, 0)), voltages, 0, STEP, coeff, table, length)
    sent = jnp.concatenate([early, later], axis=1)
    sent = sent.reshape(devices, 2, spec_dev, in_rows)
    received = lax.all_to_all(sent, ("inp", "tm"), split_axis=0, concat_axis=0, tiled=True)
    return correlate([received], groups_tm)


def solution(mesh):
    return jax.shard_map(
        per_device,
        mesh=mesh,
        in_specs=(P("inp", "tm"), P()),
        out_specs=P(("inp", "tm"), None, None, None),
        check_vma=False,
    )
```

```python
import functools
import math

import jax
import jax.numpy as jnp
import numpy as np
from jax import lax
from jax.experimental import pallas as pl
from jax.experimental.pallas import tpu as pltpu
from jax.sharding import PartitionSpec as P

CH_DEV = 1
STEP = 16
ROWS = 16
DIRECT = 2
LANES = 128
CUTS = (0, 5, 8)
VMEM_LIMIT = 60 * 1024 * 1024


def shifted(block, axis, distance):
    devices = range(lax.axis_size(axis))
    route = [(i - distance, i) for i in devices if i - distance in devices]
    return lax.ppermute(block, axis, route)


def dft_table(channels, length):
    samples = np.arange(length)
    angle = (np.arange(channels)[:, None] * samples[None, :] % length) * (2.0 * math.pi / length)
    table = np.stack([np.cos(angle), -np.sin(angle)], axis=1).reshape(2 * channels, length)
    return (table / math.sqrt(length)).T


def split_table(table):
    high = table.astype(jnp.bfloat16)
    low = (table - high.astype(np.float64)).astype(jnp.bfloat16)
    both = np.concatenate([high, low], axis=1)
    return jnp.asarray(np.concatenate([both, both], axis=0))


def tapped_table(table, coeff):
    product = coeff[:DIRECT, :, None] * jnp.asarray(table, jnp.float32)[None]
    high = lax.reduce_precision(product, exponent_bits=8, mantissa_bits=7)
    both = jnp.concatenate([high, product - high], axis=2).astype(jnp.bfloat16)
    pairs = both.reshape(DIRECT // 2, 2, *both.shape[1:])
    return jnp.concatenate([pairs[:, 0], pairs[:, 1]], axis=2)


def spectra_kernel(prev_ref, main_ref, coeff_ref, table_ref, tapped_ref, *refs, taps, length):
    in_rows = main_ref.shape[0]
    tiles = length // LANES
    groups = in_rows // ROWS
    offset = STEP
    if len(refs) > 5:
        history_ref, *refs, window_ref = refs
        offset = taps - 1

        @pl.when(pl.program_id(0) == 0)
        def _():
            window_ref[...] = history_ref[...]

        @pl.when(pl.program_id(0) > 0)
        def _():
            window_ref[...] = prev_ref[:, (STEP - offset) * length :]

        prev_ref = window_ref
    out_ref, even_ref, odd_ref, product_ref, turn_ref = refs
    width = out_ref.shape[0]

    def block_at(position, row, lane):
        ref, first = (main_ref, position) if position >= 0 else (prev_ref, position + offset)
        return ref[pl.ds(row, ROWS), first * length + lane : first * length + lane + LANES].astype(jnp.float32)

    def samples_at(position, row):
        ref, first = (main_ref, position) if position >= 0 else (prev_ref, position + offset)
        return ref[pl.ds(row, ROWS), first * length : (first + 1) * length]

    def filter_rows(group, parts_ref, lane):
        row = pl.multiple_of(group * ROWS, ROWS)
        gains = [coeff_ref[8 * j : 8 * j + 8, lane : lane + LANES] for j in range(taps)]
        sums = {}
        for position in range(1 - taps + DIRECT, STEP):
            block = block_at(position, row, lane)
            halves = [block[8 * k : 8 * k + 8] for k in range(ROWS // 8)]
            for j in range(DIRECT, taps):
                spectrum = position + taps - 1 - j
                if 0 <= spectrum < STEP:
                    terms = [gains[j] * half for half in halves]
                    if spectrum in sums:
                        terms = [s + t for s, t in zip(sums[spectrum], terms)]
                    sums[spectrum] = terms
            if position >= 0:
                total = jnp.concatenate(sums.pop(position), axis=0)
                high = total.astype(jnp.bfloat16)
                low = (total - high.astype(jnp.float32)).astype(jnp.bfloat16)
                target = slice(position * ROWS, position * ROWS + ROWS)
                parts_ref[target, lane : lane + LANES] = high
                parts_ref[target, length + lane : length + lane + LANES] = low

    def transform(group, parts_ref, part, parts):
        row = pl.multiple_of(group * ROWS, ROWS)
        count = STEP // parts
        start = part * count
        total = jnp.dot(
            parts_ref[start * ROWS : (start + count) * ROWS, :], table_ref[...], preferred_element_type=jnp.float32
        )
        columns = total.shape[1]
        for pair in range(DIRECT // 2):
            first = start + 1 - taps + 2 * pair
            samples = jnp.concatenate([samples_at(first + k, row) for k in range(count + 1)], axis=0)
            both = jnp.dot(samples, tapped_ref[pair], preferred_element_type=jnp.float32)
            total = total + both[: count * ROWS, :columns] + both[ROWS:, columns:]
        for k in range(count):
            product_ref[start + k, pl.ds(row, ROWS), :] = total[k * ROWS : k * ROWS + ROWS]

    def two_groups(pair, carry):
        before = jnp.where(pair == 0, groups - 1, 2 * pair - 1)
        for tile in range(tiles):
            filter_rows(2 * pair, even_ref, tile * LANES)
            if tile == 0:
                transform(before, odd_ref, 0, 1)
        for tile in range(tiles):
            filter_rows(2 * pair + 1, odd_ref, tile * LANES)
            if tile == 0:
                transform(2 * pair, even_ref, 0, 1)
        return carry

    lax.fori_loop(0, groups // 2, two_groups, 0)
    transform(groups - 1, odd_ref, 0, 1)

    for spectrum in range(STEP):
        product = product_ref[spectrum].T
        turn_ref[pl.ds(spectrum, width, stride=STEP), :] = product[:width] + product[width:]
    out_ref[...] = turn_ref[...].reshape(width, STEP, in_rows).astype(jnp.bfloat16)


def spectra(voltages, first, last, coeff, table, tapped, length, history):
    taps = coeff.shape[0] // 8
    in_rows = voltages.shape[0]
    width = table.shape[1] // 2
    wide = (in_rows, STEP * length)
    operands = [voltages, voltages, coeff, table, tapped]
    in_specs = [
        pl.BlockSpec(wide, lambda k: (0, jnp.maximum(k + first - 1, 0))),
        pl.BlockSpec(wide, lambda k: (0, k + first)),
        pl.BlockSpec(coeff.shape, lambda k: (0, 0)),
        pl.BlockSpec(table.shape, lambda k: (0, 0)),
        pl.BlockSpec(tapped.shape, lambda k: (0, 0, 0)),
    ]
    scratch = [
        pltpu.VMEM((STEP * ROWS, 2 * length), jnp.bfloat16),
        pltpu.VMEM((STEP * ROWS, 2 * length), jnp.bfloat16),
        pltpu.VMEM((STEP, in_rows, 2 * width), jnp.float32),
        pltpu.VMEM((width * STEP, in_rows), jnp.float32),
    ]
    if first == 0:
        operands.append(history)
        in_specs.append(pl.BlockSpec(history.shape, lambda k: (0, 0)))
        scratch.append(pltpu.VMEM(history.shape, history.dtype))
    return pl.pallas_call(
        functools.partial(spectra_kernel, taps=taps, length=length),
        grid=(last - first,),
        in_specs=in_specs,
        out_specs=pl.BlockSpec((width, STEP, in_rows), lambda k: (0, k, 0)),
        out_shape=jax.ShapeDtypeStruct((width, (last - first) * STEP, in_rows), jnp.bfloat16),
        scratch_shapes=scratch,
        compiler_params=pltpu.CompilerParams(vmem_limit_bytes=VMEM_LIMIT),
    )(*operands)


def correlate_kernel(*refs, groups_tm, scale, with_base):
    received, (out_ref, stack_ref) = refs[with_base:-2], refs[-2:]
    block = out_ref.shape[2]
    half = stack_ref.shape[0] // 2

    @pl.when(pl.program_id(0) == 0)
    def _():
        at = 0
        for part in range(2):
            for ref in received:
                sources, _, count, in_rows = ref.shape
                for source in range(sources):
                    group, slab = divmod(source, groups_tm)
                    start = at + slab * count
                    stack_ref[start : start + count, group * in_rows : (group + 1) * in_rows] = ref[source, part]
                at += groups_tm * count

    row = pl.multiple_of(pl.program_id(0) * block, block)
    turned = stack_ref[:, pl.ds(row, block)].T
    crossed = jnp.concatenate([turned[:, half:], -turned[:, :half]], axis=1)
    everything = stack_ref[...]
    for index, left in enumerate((turned, crossed)):
        total = jnp.dot(left, everything, preferred_element_type=jnp.float32) * scale
        out_ref[0, index] = total + refs[0][0, index] if with_base else total


def correlate(received, groups_tm, spectra_all, base=None):
    sources, _, _, in_rows = received[0].shape
    inputs = sources // groups_tm * in_rows
    depth = 2 * groups_tm * sum(r.shape[2] for r in received)
    block = math.gcd(inputs, LANES)
    rows = pl.BlockSpec((1, 2, block, inputs), lambda k: (0, 0, k, 0))
    bases = [] if base is None else [base]
    body = functools.partial(correlate_kernel, groups_tm=groups_tm, scale=1.0 / spectra_all, with_base=len(bases))
    return pl.pallas_call(
        body,
        grid=(inputs // block,),
        in_specs=[rows for _ in bases] + [pl.BlockSpec(r.shape, lambda k: (0, 0, 0, 0)) for r in received],
        out_specs=rows,
        out_shape=jax.ShapeDtypeStruct((1, 2, inputs, inputs), jnp.float32),
        scratch_shapes=[pltpu.VMEM((depth, inputs), jnp.bfloat16)],
        compiler_params=pltpu.CompilerParams(vmem_limit_bytes=VMEM_LIMIT),
    )(*bases, *received)


def per_device(voltages, pfb_coeff):
    in_rows = voltages.shape[0]
    taps, length = pfb_coeff.shape
    spec_dev = voltages.shape[1] // length
    groups_tm = lax.axis_size("tm")
    devices = lax.axis_size("inp") * groups_tm
    channels = CH_DEV * devices
    tail = (taps - 1) * length
    history = shifted(voltages[:, voltages.shape[1] - tail :], "tm", 1)
    coeff = jnp.repeat(pfb_coeff, 8, axis=0)
    exact = dft_table(channels, length)
    table = split_table(exact)
    tapped = tapped_table(exact, pfb_coeff)

    steps = spec_dev // STEP
    cuts = [steps - steps * share // 8 for share in CUTS]
    received = []
    for first, last in zip(cuts[1:], cuts[:-1]):
        sent = spectra(voltages, first, last, coeff, table, tapped, length, history)
        if last == steps:
            sent, history = lax.optimization_barrier((sent, history))
        sent = sent.reshape(devices, 2, sent.shape[1], in_rows)
        received.append(lax.all_to_all(sent, ("inp", "tm"), split_axis=0, concat_axis=0, tiled=True))
    spectra_all = spec_dev * groups_tm
    partial = correlate(received[:-1], groups_tm, spectra_all)
    return correlate(received[-1:], groups_tm, spectra_all, partial)


def solution(mesh):
    return jax.shard_map(
        per_device,
        mesh=mesh,
        in_specs=(P("inp", "tm"), P()),
        out_specs=P(("inp", "tm"), None, None, None),
        check_vma=False,
    )
```
